32 devices in a mesh: seq: 8 (over y, x, core), rep: 4 (over z).
Axes of the slice: x: 2, y: 2, z: 4, core: 2. Of those that a mesh axis runs over, the one named last changes fastest.
Arguments:
- query_rows: bfloat16 [8, 8, 256, 1152], P('rep', 'seq'), as said below
- key_rows: bfloat16 [8, 8, 256, 1152], P('rep', 'seq'), as said below
- value_rows: bfloat16 [8, 8, 256, 1152], P('rep', 'seq'), may hold values from -6 to 6
- out_grad: bfloat16 [8, 8, 256, 1152], P('rep', 'seq'), may hold values from -6 to 6
- out_weight: bfloat16 [1152, 1152], replicated, may hold values from -0.1875 to 0.1875
- frame_count: int32 [8], P('rep'), may hold values from 1 to 8, as said below
- pos_count: int32 [8], P('rep'), may hold values from 64 to 256, as said below
Outputs:
- projected: bfloat16 [8, 8, 256, 1152], P('rep', 'seq')
- grad_query: bfloat16 [8, 8, 256, 1152], P('rep', 'seq')
- grad_key: bfloat16 [8, 8, 256, 1152], P('rep', 'seq')
- grad_value: bfloat16 [8, 8, 256, 1152], P('rep', 'seq')
- grad_weight: float32 [1152, 1152], P('seq')
The draws below stay inside these ranges and needn't reach their ends.
Inputs may be any that keep to these rules, and one draw needn't show every extreme that they name: `query_rows`: entries lie within -40 to 40. `key_rows`: entries lie within -40 to 40. `frame_count`: some clip has all 8 frames live. `pos_count`: some clip has all 256 positions live.
All inputs are finite; a program needn't handle non-finite values.
Results may differ from the reference program's by a relative error of at most 0.0057.
Values may be sent and summed in bfloat16 or wider, within the bound.
No kernel may reach another device: no remote copies, remote signals or barrier semaphores. Data moves between devices by JAX's collectives and lax.ppermute only.
A program may use at most 128 MiB of HBM per device.

```python
import math
import jax
import jax.numpy as jnp
from jax import lax

D = 1152
HEADS = 16
POS = 256
FRAMES = 8
CLIPS = 8


def query_key_pair(key):
    base = jax.random.fold_in(key, 7)
    key_query, key_keys = jax.random.split(base, 2)
    shape_all = (CLIPS, FRAMES, POS, D)
    query_drawn = jax.random.normal(key_query, shape_all, jnp.float32)
    keys_drawn = jax.random.normal(key_keys, shape_all, jnp.float32)
    return (query_drawn, keys_drawn)


def draw_query_rows(key, part):
    return query_key_pair(key)[0].astype(jnp.bfloat16)


def draw_key_rows(key, part):
    return query_key_pair(key)[1].astype(jnp.bfloat16)


def draw_frame_count(key, part):
    key_counts, key_pick = jax.random.split(jax.random.fold_in(key, 11))
    counts = jax.random.randint(key_counts, (CLIPS,), 1, FRAMES + 1)
    chosen = jax.random.randint(key_pick, (), 0, CLIPS)
    return jnp.where(jnp.arange(CLIPS) == chosen, FRAMES, counts).astype(jnp.int32)


def draw_pos_count(key, part):
    key_counts, key_pick = jax.random.split(jax.random.fold_in(key, 13))
    counts = jax.random.randint(key_counts, (CLIPS,), POS // 4, POS + 1)
    chosen = jax.random.randint(key_pick, (), 0, CLIPS)
    return jnp.where(jnp.arange(CLIPS) == chosen, POS, counts).astype(jnp.int32)


def strengthened(result, own_key, source, target, blocks, factor):
    owner, partner = [(jnp.arange(result.shape[dim]) // (result.shape[dim] // blocks)).reshape([-1 if axis == dim else 1 for axis in range(result.ndim)]) for dim in (source, target)]
    chosen = jax.random.permutation(own_key, blocks)[partner]
    strong = (owner == chosen) | (owner == (partner + blocks // 2) % blocks)
    return jnp.where(strong, factor * result, result)


def shard_levels(rng, extent, pieces, least, high):
    def one(axis_at, shards_of):
        steps = jax.random.uniform(jax.random.fold_in(jax.random.fold_in(rng, 6), axis_at), (shards_of,), jnp.float32, least / len(pieces), high / len(pieces))
        return jnp.repeat(jnp.exp(steps), extent[axis_at] // shards_of).reshape((-1,) + (1,) * (len(extent) - axis_at - 1))

    factor_of = one(*pieces[0])
    for cut in pieces[1:]:
        factor_of = factor_of * one(*cut)
    return factor_of


def bell_draw(stream_key, dims, scale, limit, cuts=(), held_as=jnp.bfloat16):
    loudness = shard_levels(stream_key, dims, cuts, -0.22, 0.18) if cuts else 1.0
    result = jax.random.normal(stream_key, dims, jnp.float32) * scale * loudness
    return jnp.minimum(jnp.maximum(result, -limit), limit).astype(held_as)


def gaussian_with(stream_key, extent, spread, most, cuts, heavy, kind=jnp.bfloat16):
    result = spread * jax.random.normal(stream_key, extent, jnp.float32)
    if cuts:
        result = result * shard_levels(stream_key, extent, cuts, -0.22, 0.18)
    return jnp.clip(strengthened(result, jax.random.fold_in(stream_key, 3), *heavy), -most, most).astype(kind)


def setup_inputs(seed: int = 0) -> dict:
    key_list = jax.random.split(jax.random.key(seed), 8)
    return {
        "query_rows": draw_query_rows(jax.random.fold_in(key_list[7], 71), 0),
        "key_rows": draw_key_rows(jax.random.fold_in(key_list[7], 71), 0),
        "value_rows": bell_draw(key_list[2], (CLIPS, FRAMES, POS, D), 1.0, 6.0, ((0, 4), (1, 8))),
        "out_grad": gaussian_with(key_list[3], (CLIPS, FRAMES, POS, D), 1.0, 6.0, ((0, 4), (1, 8)), (1, 3, 8, 2.0)),
        "out_weight": bell_draw(key_list[4], (D, D), D ** -0.5, 0.1875),
        "frame_count": draw_frame_count(jax.random.fold_in(key_list[7], 71), 0),
        "pos_count": draw_pos_count(jax.random.fold_in(key_list[7], 71), 0),
    }


def clip_pass(query_rows, key_rows, value_rows, out_grad, out_weight, frames_live, positions_live):
    nframe, npos_all, width = query_rows.shape
    head_dim = width // HEADS
    inv_root = 1.0 / math.sqrt(head_dim)
    shape_heads = (nframe, npos_all, HEADS, head_dim)
    query_heads = query_rows.astype(jnp.float32).reshape(shape_heads)
    key_heads = key_rows.astype(jnp.float32).reshape(shape_heads)
    value_heads = value_rows.astype(jnp.float32).reshape(shape_heads)
    scores = jnp.einsum('fphd,tphd->phft', query_heads, key_heads, precision=lax.Precision.HIGHEST) * inv_root
    frame_ids = jnp.arange(nframe, dtype=jnp.int32)
    key_live = frame_ids < frames_live
    scores = jnp.where(key_live, scores, -1e+30)
    highest = lax.optimization_barrier(jnp.max(scores, axis=-1, keepdims=True))
    expo = jnp.exp(scores - highest) * key_live.astype(jnp.float32)
    weights = expo / lax.optimization_barrier(jnp.sum(expo, axis=-1, keepdims=True))
    rounded = lax.optimization_barrier(weights.astype(jnp.bfloat16)).astype(jnp.float32)
    mixed = jnp.einsum('phft,tphd->fphd', rounded, value_heads, precision=lax.Precision.HIGHEST)
    row_live = key_live[:, None] & (jnp.arange(npos_all, dtype=jnp.int32) < positions_live)[None, :]
    attn_out = jnp.where(row_live[:, :, None], mixed.reshape(nframe, npos_all, width), 0.0).astype(jnp.bfloat16)
    flat_out = attn_out.reshape(-1, width)
    flat_grad = out_grad.reshape(-1, width)
    projected = jnp.dot(flat_out, out_weight.T, preferred_element_type=jnp.float32).astype(jnp.bfloat16)
    out_cot = jnp.dot(flat_grad, out_weight, preferred_element_type=jnp.float32).reshape(nframe, npos_all, width)
    out_cot = jnp.where(row_live[:, :, None], out_cot, 0.0).astype(jnp.bfloat16)
    weight_term = lax.dot_general(flat_grad, flat_out, (((0,), (0,)), ((), ())), preferred_element_type=jnp.float32)
    cot_heads = out_cot.astype(jnp.float32).reshape(shape_heads)
    grad_value = jnp.einsum('phft,fphd->tphd', rounded, cot_heads, precision=lax.Precision.HIGHEST)
    grad_attn = jnp.einsum('fphd,tphd->phft', cot_heads, value_heads, precision=lax.Precision.HIGHEST)
    row_delta = lax.optimization_barrier(jnp.sum(weights * grad_attn, axis=-1, keepdims=True))
    grad_score = weights * (grad_attn - row_delta) * inv_root
    grad_query = jnp.einsum('phft,tphd->fphd', grad_score, key_heads, precision=lax.Precision.HIGHEST)
    grad_key = jnp.einsum('phft,fphd->tphd', grad_score, query_heads, precision=lax.Precision.HIGHEST)
    full = (nframe, npos_all, width)
    return (projected.reshape(full), grad_query.reshape(full).astype(jnp.bfloat16), grad_key.reshape(full).astype(jnp.bfloat16), grad_value.reshape(full).astype(jnp.bfloat16), weight_term)

def reference(query_rows, key_rows, value_rows, out_grad, out_weight, frame_count, pos_count):

    def advance(total, items):
        results = clip_pass(items[0], items[1], items[2], items[3], out_weight, items[4], items[5])
        return (total + results[4], results[:4])
    start_total = jnp.zeros((D, D), jnp.float32)
    total, stacked = lax.scan(advance, start_total, (query_rows, key_rows, value_rows, out_grad, frame_count, pos_count))
    return (stacked[0], stacked[1], stacked[2], stacked[3], total)
```

```python
import functools
import math

import jax
import jax.numpy as jnp
from jax import lax
from jax.experimental import pallas as pl
from jax.experimental.pallas import tpu as pltpu
from jax.sharding import PartitionSpec as P


HEADS = 16
LANES = 128
SUB = 16
VMEM = 60 * 1024 * 1024


def dot(a, b, ca, cb):
    return lax.dot_general(a, b, (((ca,), (cb,)), ((), ())), preferred_element_type=jnp.float32)


def pack_kernel(n, clip, *refs):
    ntensor = 4
    ins, outs = refs[:ntensor], refs[ntensor : ntensor + n]
    buf, sem_in, sem_out = refs[ntensor + n :]
    rank = lax.axis_index("seq")
    part = buf.shape[2]
    reads, writes = [], []
    for k in range(n):
        start = pl.multiple_of((rank ^ k) * part, part)
        for i, ref in enumerate(ins):
            copy = pltpu.make_async_copy(
                ref.at[clip, 0, pl.ds(start, part), :], buf.at[k, i], sem_in.at[k, i]
            )
            copy.start()
            reads.append(copy)
    for k in range(n):
        for i in range(ntensor):
            reads[k * ntensor + i].wait()
        copy = pltpu.make_async_copy(buf.at[k], outs[k], sem_out.at[k])
        copy.start()
        writes.append(copy)
    for copy in writes:
        copy.wait()


def pack(n, clip, tensors):
    _, _, npos, width = tensors[0].shape
    part = npos // n
    block = jax.ShapeDtypeStruct((4, part, width), jnp.bfloat16)
    return pl.pallas_call(
        functools.partial(pack_kernel, n, clip),
        out_shape=[block] * n,
        in_specs=[pl.BlockSpec(memory_space=pl.ANY)] * 4,
        out_specs=[pl.BlockSpec(memory_space=pl.ANY)] * n,
        scratch_shapes=[
            pltpu.VMEM((n, 4, part, width), jnp.bfloat16),
            pltpu.SemaphoreType.DMA((n, 4)),
            pltpu.SemaphoreType.DMA((n,)),
        ],
        compiler_params=pltpu.CompilerParams(vmem_limit_bytes=VMEM),
        name="pack",
    )(*tensors)


def unpack_kernel(n, clip, nprior, *refs):
    ins = refs[:n]
    outs = refs[n + nprior : n + nprior + 4]
    buf, sem_in, sem_out = refs[n + nprior + 4 :]
    rank = lax.axis_index("seq")
    part = buf.shape[2]
    reads, writes = [], []
    for k in range(n):
        copy = pltpu.make_async_copy(ins[k], buf.at[k], sem_in.at[k])
        copy.start()
        reads.append(copy)
    for k in range(n):
        reads[k].wait()
        start = pl.multiple_of((rank ^ k) * part, part)
        for i, ref in enumerate(outs):
            copy = pltpu.make_async_copy(
                buf.at[k, i], ref.at[clip, 0, pl.ds(start, part), :], sem_out.at[k, i]
            )
            copy.start()
            writes.append(copy)
    for copy in writes:
        copy.wait()


def unpack(n, clip, full, blocks, prior):
    part, width = blocks[0].shape[1:]
    nprior = len(prior)
    return pl.pallas_call(
        functools.partial(unpack_kernel, n, clip, nprior),
        out_shape=[jax.ShapeDtypeStruct(full, jnp.bfloat16)] * 4,
        in_specs=[pl.BlockSpec(memory_space=pl.ANY)] * (n + nprior),
        out_specs=[pl.BlockSpec(memory_space=pl.ANY)] * 4,
        input_output_aliases={n + i: i for i in range(nprior)},
        scratch_shapes=[
            pltpu.VMEM((n, 4, part, width), jnp.bfloat16),
            pltpu.SemaphoreType.DMA((n,)),
            pltpu.SemaphoreType.DMA((n, 4)),
        ],
        compiler_params=pltpu.CompilerParams(vmem_limit_bytes=VMEM),
        name="unpack",
    )(*blocks, *prior)


def attend_kernel(n, clip, last, nprior, frames_ref, places_ref, *refs):
    ins, weight_ref = refs[:n], refs[n]
    prior = refs[n + 1 : n + 1 + nprior]
    refs = refs[n + 1 + nprior :]
    outs, refs = refs[:n], refs[n:]
    wgrads, refs = refs[: 1 + last], refs[1 + last :]
    q_s, k_s, v_s, g_s, c_s, o_s, dq_s, dk_s, dv_s, pr_s, w_s, gw_s = refs[:12]
    sem_in, sem_w, sem_out, sem_gw = refs[12:]
    rank = lax.axis_index("seq")
    part, width = ins[0].shape[1:]
    nblock = part // SUB
    rows = n * SUB
    head_dim = width // HEADS
    inv_root = 1.0 / math.sqrt(head_dim)
    nframe_live = frames_ref[clip]
    nplace_live = places_ref[clip]

    reads = {}
    for i, ref in ((3, g_s), (0, q_s), (1, k_s), (2, v_s)):
        reads[i] = [
            pltpu.make_async_copy(
                ins[k].at[i, pl.ds(b * SUB, SUB), :],
                ref.at[b, pl.ds(k * SUB, SUB), :],
                sem_in.at[i, b, k],
            )
            for b in range(nblock)
            for k in range(n)
        ]
    weight_read = pltpu.make_async_copy(weight_ref, w_s, sem_w.at[0])
    weight_read.start()
    for i in (3, 0, 1, 2):
        for copy in reads[i]:
            copy.start()
    prior_reads = [pltpu.make_async_copy(ref, gw_s, sem_w.at[1]) for ref in prior]
    for copy in prior_reads:
        copy.start()

    row_id = lax.broadcasted_iota(jnp.int32, (rows, 1), 0)
    col_id = lax.broadcasted_iota(jnp.int32, (1, rows), 1)
    row_alive = ((row_id // SUB) ^ rank) < nframe_live
    key_alive = ((col_id // SUB) ^ rank) < nframe_live
    allowed = ((row_id % SUB) == (col_id % SUB)) & key_alive

    def live(b):
        place = rank * part + b * SUB + row_id % SUB
        return row_alive & (place < nplace_live)

    weight_read.wait()
    for copy in reads[3]:
        copy.wait()
    for b in range(nblock):
        cot = dot(g_s[b], w_s[...], 1, 0)
        c_s[b] = jnp.where(live(b), cot, 0.0).astype(jnp.bfloat16)
    for i in (0, 1, 2):
        for copy in reads[i]:
            copy.wait()

    window_lane = lax.broadcasted_iota(jnp.int32, (1, 2 * LANES), 1)

    def pairs(b, carry):
        alive = live(b)
        for j in range(HEADS // 2):
            lanes = slice(j * LANES, (j + 2) * LANES)
            first = 2 * head_dim * j - LANES * j
            own = [
                (window_lane >= first + h * head_dim) & (window_lane < first + (h + 1) * head_dim)
                for h in range(2)
            ]

            def both(x):
                zero = jnp.zeros_like(x)
                return jnp.concatenate([jnp.where(m, x, zero) for m in own], axis=0)

            qw, kw, vw, cw = q_s[b, :, lanes], k_s[b, :, lanes], v_s[b, :, lanes], c_s[b, :, lanes]
            q2, k2, v2, c2 = both(qw), both(kw), both(vw), both(cw)
            scores = dot(qw, k2, 1, 1)
            gattns = dot(cw, v2, 1, 1)
            rounded, high, low = [], [], []
            for h in range(2):
                part_of = slice(h * rows, (h + 1) * rows)
                score = jnp.where(allowed, scores[:, part_of] * inv_root, -1e30)
                expo = jnp.exp(score - jnp.max(score, axis=1, keepdims=True))
                weights = expo / jnp.sum(expo, axis=1, keepdims=True)
                rounded.append(weights.astype(jnp.bfloat16))
                gattn = gattns[:, part_of]
                delta = jnp.sum(weights * gattn, axis=1, keepdims=True)
                gscore = weights * (gattn - delta) * inv_root
                high.append(gscore.astype(jnp.bfloat16))
                low.append((gscore - high[h].astype(jnp.float32)).astype(jnp.bfloat16))
            across = [jnp.concatenate(x, axis=1) for x in (rounded, high, low)]
            down = [jnp.concatenate(x, axis=0) for x in (rounded, high, low)]
            out = jnp.where(alive, dot(across[0], v2, 1, 0), 0.0)
            dq = dot(across[1], k2, 1, 0) + dot(across[2], k2, 1, 0)
            dv = dot(down[0], c2, 0, 0)
            dk = dot(down[1], q2, 0, 0) + dot(down[2], q2, 0, 0)
            mine = window_lane[:, :LANES] >= first
            lead = slice(j * LANES, (j + 1) * LANES)
            tail = slice((j + 1) * LANES, (j + 2) * LANES)
            for ref, value in ((o_s, out), (dq_s, dq), (dk_s, dk), (dv_s, dv)):
                value = value.astype(jnp.bfloat16)
                if j:
                    ref[b, :, lead] = jnp.where(mine, value[:, :LANES], ref[b, :, lead])
                else:
                    ref[b, :, lead] = value[:, :LANES]
                ref[b, :, tail] = value[:, LANES:]
        return carry

    lax.fori_loop(0, nblock, pairs, 0)

    writes = []

    def send(i, ref):
        for k in range(n):
            for b in range(nblock):
                copy = pltpu.make_async_copy(
                    ref.at[b, pl.ds(k * SUB, SUB), :],
                    outs[k].at[i, pl.ds(b * SUB, SUB), :],
                    sem_out.at[i, b, k],
                )
                copy.start()
                writes.append(copy)

    for i, ref in ((1, dq_s), (2, dk_s), (3, dv_s)):
        send(i, ref)
    for copy in prior_reads:
        copy.wait()
    tile = width // 3
    for i in range(3):
        cols = slice(i * tile, (i + 1) * tile)
        total = gw_s[cols, :] if nprior else 0.0
        for b in range(nblock):
            total = total + dot(g_s[b, :, cols], o_s[b], 0, 0)
        gw_s[cols, :] = total
    if last:
        half, count = n // 2, width // n
        give, keep = wgrads
        core = rank % 2
        for m in range(half):
            there = pl.multiple_of((2 * m + 1 - core) * count, 8)
            give[m] = gw_s[pl.ds(there, count), :].astype(jnp.bfloat16)
            here = pl.multiple_of((2 * m + core) * count, 8)
            copy = pltpu.make_async_copy(gw_s.at[pl.ds(here, count), :], keep.at[m], sem_gw.at[m])
            copy.start()
            writes.append(copy)
    else:
        copy = pltpu.make_async_copy(gw_s, wgrads[0], sem_gw.at[0])
        copy.start()
        writes.append(copy)
    for b in range(nblock):
        pr_s[b] = dot(o_s[b], w_s[...], 1, 1).astype(jnp.bfloat16)
    send(0, pr_s)
    for copy in writes:
        copy.wait()


def attend(n, clip, last, frame_count, pos_count, blocks, weight, prior):
    part, width = blocks[0].shape[1:]
    nblock, rows = part // SUB, n * SUB
    vmem = pl.BlockSpec(memory_space=pltpu.VMEM)
    smem = pl.BlockSpec(memory_space=pltpu.SMEM)
    hbm = pl.BlockSpec(memory_space=pl.ANY)
    nprior = len(prior)
    block = jax.ShapeDtypeStruct((4, part, width), jnp.bfloat16)
    if last:
        halves = (n // 2, width // n, width)
        wgrads = [jax.ShapeDtypeStruct(halves, t) for t in (jnp.bfloat16, jnp.float32)]
        wspecs = [vmem, hbm]
    else:
        wgrads, wspecs = [jax.ShapeDtypeStruct((width, width), jnp.float32)], [hbm]
    return pl.pallas_call(
        functools.partial(attend_kernel, n, clip, last, nprior),
        out_shape=[block] * n + wgrads,
        in_specs=[smem, smem] + [hbm] * (n + 1 + nprior),
        out_specs=[hbm] * n + wspecs,
        scratch_shapes=[pltpu.VMEM((nblock, rows, width), jnp.bfloat16)] * 10
        + [
            pltpu.VMEM((width, width), jnp.bfloat16),
            pltpu.VMEM((width, width), jnp.float32),
            pltpu.SemaphoreType.DMA((4, nblock, n)),
            pltpu.SemaphoreType.DMA((2,)),
            pltpu.SemaphoreType.DMA((4, nblock, n)),
            pltpu.SemaphoreType.DMA((n // 2,)),
        ],
        compiler_params=pltpu.CompilerParams(vmem_limit_bytes=VMEM),
        cost_estimate=pl.CostEstimate(
            flops=10_000_000_000, bytes_accessed=16_000_000, transcendentals=0
        ),
        name="attend",
    )(frame_count, pos_count, *blocks, weight, *prior)


def small_call(kernel, out_shape, args, scratch=()):
    vmem = pl.BlockSpec(memory_space=pltpu.VMEM)
    return pl.pallas_call(
        kernel,
        out_shape=out_shape,
        in_specs=[vmem] * len(args),
        out_specs=[vmem] * len(out_shape),
        scratch_shapes=list(scratch),
        compiler_params=pltpu.CompilerParams(vmem_limit_bytes=VMEM),
        cost_estimate=pl.CostEstimate(
            flops=1_000_000_000, bytes_accessed=4_000_000, transcendentals=0
        ),
    )(*args)


def chip_sum_kernel(half, keep, came, own, *outs):
    chip = lax.axis_index("seq") // 2
    own[...] = keep[chip] + came[chip].astype(jnp.float32)
    for q in range(1, half):
        outs[q - 1][...] = (keep[chip ^ q] + came[chip ^ q].astype(jnp.float32)).astype(jnp.bfloat16)


def plane_sum_kernel(half, nrep, own, *refs):
    came, mine, outs, acc = refs[: half - 1], refs[half - 1], refs[half:-1], refs[-1]
    plane = lax.axis_index("rep")
    count, share = own.shape[0], mine.shape[0]
    acc[...] = jnp.zeros_like(acc)
    total = own[...]
    for ref in came:
        total = total + ref[...].astype(jnp.float32)
    acc[:count, :] = total
    mine[...] = acc[pl.ds(pl.multiple_of(plane * share, 8), share), :]
    for w in range(1, nrep):
        there = pl.multiple_of((plane ^ w) * share, 8)
        outs[w - 1][...] = acc[pl.ds(there, share), :].astype(jnp.bfloat16)


def replica_sum_kernel(mine, *refs):
    total = mine[...]
    for ref in refs[:-1]:
        total = total + ref[...].astype(jnp.float32)
    refs[-1][...] = total.astype(jnp.bfloat16)


def assemble_kernel(nrep, *refs):
    parts, out, acc = refs[:nrep], refs[-2], refs[-1]
    plane = lax.axis_index("rep")
    share = parts[0].shape[0]
    for w in range(nrep):
        there = pl.multiple_of((plane ^ w) * share, 8)
        acc[pl.ds(there, share), :] = parts[w][...].astype(jnp.float32)
    out[...] = acc[: out.shape[0], :]


def permute(x, axis, size, step):
    return lax.ppermute(x, axis, [(i, i ^ step) for i in range(size)])


def exchange(n, order, blocks):
    moved = [None] * n
    moved[0] = blocks[0]
    for k in order:
        moved[k] = permute(blocks[k], "seq", n, k)
    return moved


def reduce_weight(n, nrep, give, keep):
    half, count, width = keep.shape
    came = permute(give, "seq", n, 1)
    wide = jax.ShapeDtypeStruct((count, width), jnp.float32)
    narrow = jax.ShapeDtypeStruct((count, width), jnp.bfloat16)
    own, *sends = small_call(
        functools.partial(chip_sum_kernel, half), [wide] + [narrow] * (half - 1), [keep, came]
    )
    came = [permute(sends[q - 1], "seq", n, 2 * q) for q in range(1, half)]
    share = -(-(-(-count // nrep)) // 8) * 8
    acc = pltpu.VMEM((nrep * share, width), jnp.float32)
    wide = jax.ShapeDtypeStruct((share, width), jnp.float32)
    narrow = jax.ShapeDtypeStruct((share, width), jnp.bfloat16)
    mine, *sends = small_call(
        functools.partial(plane_sum_kernel, half, nrep),
        [wide] + [narrow] * (nrep - 1),
        [own, *came],
        [acc],
    )
    came = [permute(sends[w - 1], "rep", nrep, w) for w in range(1, nrep)]
    (mine,) = small_call(replica_sum_kernel, [narrow], [mine, *came])
    came = [permute(mine, "rep", nrep, w) for w in range(1, nrep)]
    (out,) = small_call(
        functools.partial(assemble_kernel, nrep),
        [jax.ShapeDtypeStruct((count, width), jnp.float32)],
        [mine, *came],
        [acc],
    )
    return out


def send_order(n):
    return sorted(range(1, n), key=lambda k: (k < 2, -bin(k >> 1).count("1"), k))


def shards(n, nrep, query_rows, key_rows, value_rows, out_grad, out_weight, frame_count, pos_count):
    nclip, frame_local, npos, _ = query_rows.shape
    if frame_local != 1 or n & (n - 1) or nrep & (nrep - 1) or (npos // n) % SUB:
        raise ValueError("sizes")
    order = send_order(n)
    tensors = (query_rows, key_rows, value_rows, out_grad)
    arrived = [exchange(n, order, pack(n, c, tensors)) for c in range(nclip)]
    prior, back = (), []
    for c in range(nclip):
        last = c == nclip - 1
        done = attend(n, c, last, frame_count, pos_count, arrived[c], out_weight, prior)
        blocks, prior = done[:n], tuple(done[n:])
        back.append(exchange(n, order, blocks))
    wgrad = reduce_weight(n, nrep, *prior)
    outs = ()
    for c in range(nclip):
        outs = unpack(n, c, query_rows.shape, back[c], outs)
    return (*outs, wgrad)


def solution(mesh):
    n, nrep = mesh.shape["seq"], mesh.shape["rep"]
    rows = P("rep", "seq", None, None)
    return jax.shard_map(
        functools.partial(shards, n, nrep),
        mesh=mesh,
        in_specs=(rows, rows, rows, rows, P(), P("rep"), P("rep")),
        out_specs=(rows, rows, rows, rows, P("seq", None)),
        check_vma=False,
    )
```

```python
import functools
import math

import jax
import jax.numpy as jnp
from jax import lax
from jax.experimental import pallas as pl
from jax.experimental.pallas import tpu as pltpu
from jax.sharding import PartitionSpec as P


HEADS = 16
LANES = 128
SUB = 16
VMEM = 60 * 1024 * 1024


def dot(a, b, ca, cb):
    return lax.dot_general(a, b, (((ca,), (cb,)), ((), ())), preferred_element_type=jnp.float32)


def pack_kernel(n, clip, low, slots, *refs):
    ntensor, count = 4, len(slots)
    ins, outs = refs[:ntensor], refs[ntensor : ntensor + count]
    buf, sem_in, sem_out = refs[ntensor + count :]
    rank = lax.axis_index("seq")
    part, size = ins[0].shape[2] // n, buf.shape[2]
    reads, writes = [], []
    for j, k in enumerate(slots):
        start = pl.multiple_of((rank ^ k) * part + low, SUB)
        for i, ref in enumerate(ins):
            copy = pltpu.make_async_copy(
                ref.at[clip, 0, pl.ds(start, size), :], buf.at[j, i], sem_in.at[j, i]
            )
            copy.start()
            reads.append(copy)
    for j in range(count):
        for i in range(ntensor):
            reads[j * ntensor + i].wait()
        copy = pltpu.make_async_copy(buf.at[j], outs[j], sem_out.at[j])
        copy.start()
        writes.append(copy)
    for copy in writes:
        copy.wait()


def pack(n, slots, clip, low, size, tensors):
    width, count = tensors[0].shape[3], len(slots)
    block = jax.ShapeDtypeStruct((4, size, width), jnp.bfloat16)
    outs = pl.pallas_call(
        functools.partial(pack_kernel, n, clip, low, slots),
        out_shape=[block] * count,
        in_specs=[pl.BlockSpec(memory_space=pl.ANY)] * 4,
        out_specs=[pl.BlockSpec(memory_space=pl.ANY)] * count,
        scratch_shapes=[
            pltpu.VMEM((count, 4, size, width), jnp.bfloat16),
            pltpu.SemaphoreType.DMA((count, 4)),
            pltpu.SemaphoreType.DMA((count,)),
        ],
        compiler_params=pltpu.CompilerParams(vmem_limit_bytes=VMEM),
        name="pack",
    )(*tensors)
    return dict(zip(slots, outs))


def unpack_kernel(n, clip, low, nprior, *refs):
    ins = refs[:n]
    outs = refs[n + nprior : n + nprior + 4]
    buf, sem_in, sem_out = refs[n + nprior + 4 :]
    rank = lax.axis_index("seq")
    part, size = outs[0].shape[2] // n, buf.shape[2]
    reads, writes = [], []
    for k in range(n):
        copy = pltpu.make_async_copy(ins[k], buf.at[k], sem_in.at[k])
        copy.start()
        reads.append(copy)
    for k in range(n):
        reads[k].wait()
        start = pl.multiple_of((rank ^ k) * part + low, SUB)
        for i, ref in enumerate(outs):
            copy = pltpu.make_async_copy(
                buf.at[k, i], ref.at[clip, 0, pl.ds(start, size), :], sem_out.at[k, i]
            )
            copy.start()
            writes.append(copy)
    for copy in writes:
        copy.wait()


def unpack(n, clip, low, full, blocks, prior):
    part, width = blocks[0].shape[1:]
    nprior = len(prior)
    return pl.pallas_call(
        functools.partial(unpack_kernel, n, clip, low, nprior),
        out_shape=[jax.ShapeDtypeStruct(full, jnp.bfloat16)] * 4,
        in_specs=[pl.BlockSpec(memory_space=pl.ANY)] * (n + nprior),
        out_specs=[pl.BlockSpec(memory_space=pl.ANY)] * 4,
        input_output_aliases={n + i: i for i in range(nprior)},
        scratch_shapes=[
            pltpu.VMEM((n, 4, part, width), jnp.bfloat16),
            pltpu.SemaphoreType.DMA((n,)),
            pltpu.SemaphoreType.DMA((n, 4)),
        ],
        compiler_params=pltpu.CompilerParams(vmem_limit_bytes=VMEM),
        name="unpack",
    )(*blocks, *prior)


def attend_kernel(n, clip, low, share, last, nprior, frames_ref, places_ref, *refs):
    ins, weight_ref = refs[:n], refs[n]
    prior, refs = refs[n + 1 : n + 1 + nprior], refs[n + 1 + nprior :]
    outs, refs = refs[:n], refs[n:]
    extra, refs = refs[: 1 + last], refs[1 + last :]
    x_s, y_s, c_s, o_s, w_s, gw_s, sem_in, sem_w, sem_out, sem_gw = refs
    rank = lax.axis_index("seq")
    part, width = ins[0].shape[1:]
    nblock = part // SUB
    rows = n * SUB
    every = n * part
    head_dim = width // HEADS
    inv_root = 1.0 / math.sqrt(head_dim)
    nframe_live = frames_ref[clip]
    nplace_live = places_ref[clip] - (rank * share + low)

    reads = [pltpu.make_async_copy(weight_ref, w_s, sem_w.at[0])]
    reads += [pltpu.make_async_copy(ins[k], x_s.at[k], sem_in.at[k]) for k in range(n)]
    prior_reads = [pltpu.make_async_copy(ref, gw_s, sem_w.at[1]) for ref in prior]
    for copy in reads:
        copy.start()

    def frame(row):
        return (row // part) ^ rank

    row_id = lax.broadcasted_iota(jnp.int32, (every, 1), 0)
    alive = (frame(row_id) < nframe_live) & (row_id % part < nplace_live)
    key_id = lax.broadcasted_iota(jnp.int32, (rows, 1), 0)
    query_id = lax.broadcasted_iota(jnp.int32, (1, rows), 1)
    key_alive = ((key_id // SUB) ^ rank) < nframe_live
    allowed = ((key_id % SUB) == (query_id % SUB)) & key_alive
    block_alive = ((key_id // SUB) ^ rank) < nframe_live

    for copy in reads:
        copy.wait()
    for copy in prior_reads:
        copy.start()
    grad = x_s[:, 3].reshape(every, width)
    cot = jnp.where(alive, dot(grad, w_s[...], 1, 0), 0.0).astype(jnp.bfloat16)
    c_s[...] = cot.reshape(n, part, width)

    window_lane = lax.broadcasted_iota(jnp.int32, (1, 2 * LANES), 1)

    def pairs(b, carry):
        these = pl.ds(pl.multiple_of(b * SUB, SUB), SUB)
        live = block_alive & (b * SUB + key_id % SUB < nplace_live)
        for j in range(HEADS // 2):
            lanes = slice(j * LANES, (j + 2) * LANES)
            first = 2 * head_dim * j - LANES * j
            own = [
                (window_lane >= first + h * head_dim) & (window_lane < first + (h + 1) * head_dim)
                for h in range(2)
            ]

            def both(x):
                zero = jnp.zeros_like(x)
                return jnp.concatenate([jnp.where(m, x, zero) for m in own], axis=0)

            qw, kw, vw = (x_s[:, i, these, lanes].reshape(rows, 2 * LANES) for i in range(3))
            cw = c_s[:, these, lanes].reshape(rows, 2 * LANES)
            q2, k2, v2, c2 = both(qw), both(kw), both(vw), both(cw)
            scores = dot(k2, qw, 1, 1)
            gattns = dot(v2, cw, 1, 1)
            rounded, high, low = [], [], []
            for h in range(2):
                part_of = slice(h * rows, (h + 1) * rows)
                score = jnp.where(allowed, scores[part_of] * inv_root, -1e30)
                expo = jnp.exp(score - jnp.max(score, axis=0, keepdims=True))
                weights = expo * (1.0 / jnp.sum(expo, axis=0, keepdims=True))
                rounded.append(weights.astype(jnp.bfloat16))
                gattn = gattns[part_of]
                delta = jnp.sum(weights * gattn, axis=0, keepdims=True)
                gscore = weights * ((gattn - delta) * inv_root)
                high.append(gscore.astype(jnp.bfloat16))
                low.append((gscore - high[h].astype(jnp.float32)).astype(jnp.bfloat16))
            across = [jnp.concatenate(x, axis=1) for x in (rounded, high, low)]
            down = [jnp.concatenate(x, axis=0) for x in (rounded, high, low)]
            out = jnp.where(live, dot(down[0], v2, 0, 0), 0.0)
            dq = dot(down[1], k2, 0, 0) + dot(down[2], k2, 0, 0)
            dv = dot(across[0], c2, 1, 0)
            dk = dot(across[1], q2, 1, 0) + dot(across[2], q2, 1, 0)
            mine = window_lane[:, :LANES] >= first
            lead = slice(j * LANES, (j + 1) * LANES)
            tail = slice((j + 1) * LANES, (j + 2) * LANES)
            targets = [o_s] + [y_s.at[:, i] for i in (1, 2, 3)]
            for ref, value in zip(targets, (out, dq, dk, dv)):
                value = value.astype(jnp.bfloat16).reshape(n, SUB, 2 * LANES)
                if j:
                    ref[:, these, lead] = jnp.where(mine[None], value[:, :, :LANES], ref[:, these, lead])
                else:
                    ref[:, these, lead] = value[:, :, :LANES]
                ref[:, these, tail] = value[:, :, LANES:]
        return carry

    lax.fori_loop(0, nblock, pairs, 0)

    writes = []

    def send(source, target, sem):
        copy = pltpu.make_async_copy(source, target, sem)
        copy.start()
        writes.append(copy)

    for k in range(n):
        send(y_s.at[k, pl.ds(1, 3)], outs[k].at[pl.ds(1, 3)], sem_out.at[1, k])
    for copy in prior_reads:
        copy.wait()
    tile = width // 3
    for i in range(3):
        cols = slice(i * tile, (i + 1) * tile)
        total = dot(x_s[:, 3, :, cols].reshape(every, tile), o_s[...].reshape(every, width), 0, 0)
        gw_s[cols, :] = gw_s[cols, :] + total if nprior else total
    if last:
        half, count = n // 2, width // n
        give, keep = extra
        core = rank % 2
        for m in range(half):
            here = pl.multiple_of((2 * m + core) * count, 8)
            keep[m] = gw_s[pl.ds(here, count), :].astype(jnp.bfloat16)
            there = pl.multiple_of((2 * m + 1 - core) * count, 8)
            give[m] = gw_s[pl.ds(there, count), :].astype(jnp.bfloat16)
    else:
        send(gw_s, extra[0], sem_gw.at[0])
    projected = dot(o_s[...].reshape(every, width), w_s[...], 1, 1).astype(jnp.bfloat16)
    y_s[:, 0] = projected.reshape(n, part, width)
    for k in range(n):
        send(y_s.at[k, 0], outs[k].at[0], sem_out.at[0, k])
    for copy in writes:
        copy.wait()


def attend(n, clip, low, share, last, frame_count, pos_count, blocks, weight, prior):
    part, width = blocks[0].shape[1:]
    vmem = pl.BlockSpec(memory_space=pltpu.VMEM)
    smem = pl.BlockSpec(memory_space=pltpu.SMEM)
    hbm = pl.BlockSpec(memory_space=pl.ANY)
    nprior = len(prior)
    block = jax.ShapeDtypeStruct((4, part, width), jnp.bfloat16)
    if last:
        halves = (n // 2, width // n, width)
        extra = [jax.ShapeDtypeStruct(halves, jnp.bfloat16)] * 2
        espec = [vmem, vmem]
    else:
        extra, espec = [jax.ShapeDtypeStruct((width, width), jnp.float32)], [hbm]
    return pl.pallas_call(
        functools.partial(attend_kernel, n, clip, low, share, last, nprior),
        out_shape=[block] * n + extra,
        in_specs=[smem, smem] + [hbm] * (n + 1 + nprior),
        out_specs=[hbm] * n + espec,
        scratch_shapes=[
            pltpu.VMEM((n, 4, part, width), jnp.bfloat16),
            pltpu.VMEM((n, 4, part, width), jnp.bfloat16),
            pltpu.VMEM((n, part, width), jnp.bfloat16),
            pltpu.VMEM((n, part, width), jnp.bfloat16),
            pltpu.VMEM((width, width), jnp.bfloat16),
            pltpu.VMEM((width, width), jnp.float32),
            pltpu.SemaphoreType.DMA((n,)),
            pltpu.SemaphoreType.DMA((2,)),
            pltpu.SemaphoreType.DMA((2, n)),
            pltpu.SemaphoreType.DMA((n // 2,)),
        ],
        compiler_params=pltpu.CompilerParams(vmem_limit_bytes=VMEM),
        cost_estimate=pl.CostEstimate(
            flops=10_000_000_000, bytes_accessed=16_000_000, transcendentals=0
        ),
        name="attend",
    )(frame_count, pos_count, *blocks, weight, *prior)


def small_call(kernel, out_shape, args, scratch=()):
    vmem = pl.BlockSpec(memory_space=pltpu.VMEM)
    return pl.pallas_call(
        kernel,
        out_shape=out_shape,
        in_specs=[vmem] * len(args),
        out_specs=[vmem] * len(out_shape),
        scratch_shapes=list(scratch),
        compiler_params=pltpu.CompilerParams(vmem_limit_bytes=VMEM),
        cost_estimate=pl.CostEstimate(
            flops=1_000_000_000, bytes_accessed=4_000_000, transcendentals=0
        ),
    )(*args)


def chip_sum_kernel(half, keep, came, own, *outs):
    chip = lax.axis_index("seq") // 2
    own[...] = keep[chip].astype(jnp.float32) + came[chip].astype(jnp.float32)
    for q in range(1, half):
        total = keep[chip ^ q].astype(jnp.float32) + came[chip ^ q].astype(jnp.float32)
        outs[q - 1][...] = total.astype(jnp.bfloat16)


def plane_sum_kernel(half, nrep, own, *refs):
    came, mine, outs, acc = refs[: half - 1], refs[half - 1], refs[half:-1], refs[-1]
    plane = lax.axis_index("rep")
    count, share = own.shape[0], mine.shape[0]
    acc[...] = jnp.zeros_like(acc)
    total = own[...]
    for ref in came:
        total = total + ref[...].astype(jnp.float32)
    acc[:count, :] = total
    mine[...] = acc[pl.ds(pl.multiple_of(plane * share, 8), share), :]
    for w in range(1, nrep):
        there = pl.multiple_of((plane ^ w) * share, 8)
        outs[w - 1][...] = acc[pl.ds(there, share), :].astype(jnp.bfloat16)


def replica_sum_kernel(mine, *refs):
    total = mine[...]
    for ref in refs[:-1]:
        total = total + ref[...].astype(jnp.float32)
    refs[-1][...] = total.astype(jnp.bfloat16)


def assemble_kernel(nrep, *refs):
    parts, out, acc = refs[:nrep], refs[-2], refs[-1]
    plane = lax.axis_index("rep")
    share = parts[0].shape[0]
    for w in range(nrep):
        there = pl.multiple_of((plane ^ w) * share, 8)
        acc[pl.ds(there, share), :] = parts[w][...].astype(jnp.float32)
    out[...] = acc[: out.shape[0], :]


def permute(x, axis, size, step):
    return lax.ppermute(x, axis, [(i, i ^ step) for i in range(size)])


def exchange(n, order, blocks):
    moved = [None] * n
    moved[0] = blocks[0]
    for k in order:
        moved[k] = permute(blocks[k], "seq", n, k)
    return moved


def reduce_weight(n, nrep, give, keep):
    half, count, width = keep.shape
    came = permute(give, "seq", n, 1)
    wide = jax.ShapeDtypeStruct((count, width), jnp.float32)
    narrow = jax.ShapeDtypeStruct((count, width), jnp.bfloat16)
    own, *sends = small_call(
        functools.partial(chip_sum_kernel, half), [wide] + [narrow] * (half - 1), [keep, came]
    )
    came = [permute(sends[q - 1], "seq", n, 2 * q) for q in range(1, half)]
    share = -(-(-(-count // nrep)) // 8) * 8
    acc = pltpu.VMEM((nrep * share, width), jnp.float32)
    wide = jax.ShapeDtypeStruct((share, width), jnp.float32)
    narrow = jax.ShapeDtypeStruct((share, width), jnp.bfloat16)
    mine, *sends = small_call(
        functools.partial(plane_sum_kernel, half, nrep),
        [wide] + [narrow] * (nrep - 1),
        [own, *came],
        [acc],
    )
    came = [permute(sends[w - 1], "rep", nrep, w) for w in range(1, nrep)]
    (mine,) = small_call(replica_sum_kernel, [narrow], [mine, *came])
    came = [permute(mine, "rep", nrep, w) for w in range(1, nrep)]
    (out,) = small_call(
        functools.partial(assemble_kernel, nrep),
        [jax.ShapeDtypeStruct((count, width), jnp.float32)],
        [mine, *came],
        [acc],
    )
    return out


def send_order(n):
    return sorted(range(1, n), key=lambda k: (k < 2, -bin(k >> 1).count("1"), k))


def plan(nclip, share):
    return [(c, 0, share) for c in range(nclip)]


def shards(n, nrep, query_rows, key_rows, value_rows, out_grad, out_weight, frame_count, pos_count):
    nclip, frame_local, npos, _ = query_rows.shape
    if frame_local != 1 or n & (n - 1) or nrep & (nrep - 1) or (npos // n) % SUB:
        raise ValueError("sizes")
    order = send_order(n)
    tensors = (query_rows, key_rows, value_rows, out_grad)
    share = npos // n
    chunks = plan(nclip, share)
    arrived = []
    for chunk in chunks:
        blocks = {}
        for slots in (order[:2], order[2:] + [0]):
            blocks.update(pack(n, slots, *chunk, tensors))
        arrived.append(exchange(n, order, blocks))
    extra, back = (), []
    for c, (clip, low, _) in enumerate(chunks):
        last = c == len(chunks) - 1
        done = attend(
            n, clip, low, share, last, frame_count, pos_count, arrived[c], out_weight, extra
        )
        blocks, extra = done[:n], done[n:]
        back.append(exchange(n, order, blocks))
    wgrad = reduce_weight(n, nrep, *extra)
    outs = ()
    for c, (clip, low, _) in enumerate(chunks):
        outs = unpack(n, clip, low, query_rows.shape, back[c], outs)
    return (*outs, wgrad)


def solution(mesh):
    n, nrep = mesh.shape["seq"], mesh.shape["rep"]
    rows = P("rep", "seq", None, None)
    return jax.shard_map(
        functools.partial(shards, n, nrep),
        mesh=mesh,
        in_specs=(rows, rows, rows, rows, P(), P("rep"), P("rep")),
        out_specs=(rows, rows, rows, rows, P("seq", None)),
        check_vma=False,
    )
```
